32 devices in a mesh: seq: 16 (over z, y, x), head: 2 (over core).
Axes of the slice: x: 2, y: 2, z: 4, core: 2. Of those that a mesh axis runs over, the one named last changes fastest.
Arguments:
- tokens: bfloat16 [16384, 2048], P('seq'), may hold values from -6 to 6
- w_query: bfloat16 [2048, 256], P(None, 'head'), may hold values from -0.25 to 0.25
- w_key: bfloat16 [2048, 256], P(None, 'head'), may hold values from -0.25 to 0.25
- w_value: bfloat16 [2048, 2048], P(None, 'head'), may hold values from -0.125 to 0.125
- w_out: bfloat16 [2048, 2048], replicated, may hold values from -1.796875 to 1.796875
Outputs:
- mixed: bfloat16 [16384, 2048], P('seq', 'head')
The draws below stay inside these ranges and needn't reach their ends.
All inputs are finite; a program needn't handle non-finite values.
Results may differ from the reference program's by a relative error of at most 0.011.
Values may be sent and summed in bfloat16 or wider, within the bound.
A program may use at most 128 MiB of HBM per device.

```python
import jax
import jax.numpy as jnp
from jax import lax

D = 2048
HEADS = 16
KEY_DIM = 16
VALUE_DIM = 128
TOK_DEV = 1024
FEATURES = 273
TOKENS = 16384
N_SEQ = 16


def steps_of(stream_key, extent, split, least, largest):
    factor_of, own = 1.0, jax.random.fold_in(stream_key, 6)
    for axis_at, shards_of in split:
        draws = jnp.exp(jax.random.uniform(jax.random.fold_in(own, axis_at), (shards_of,), jnp.float32, least / len(split), largest / len(split)))
        factor_of = factor_of * jnp.repeat(draws, extent[axis_at] // shards_of).reshape([-1 if axis == axis_at else 1 for axis in range(len(extent))])
    return factor_of


def normal_values(own_key, dims, spread, most, split=(), held_as=jnp.bfloat16):
    result = spread * jax.random.normal(own_key, dims, jnp.float32)
    if split:
        result = result * steps_of(own_key, dims, split, -0.22, 0.18)
    return jnp.clip(result, -most, most).astype(held_as)


def setup_inputs(seed: int = 0) -> dict:
    seeds = jax.random.split(jax.random.key(seed), 6)
    tokens = normal_values(seeds[0], (TOKENS, D), 1.0, 6.0, ((0, 16),))
    w_query = normal_values(seeds[1], (D, HEADS * KEY_DIM), (D // 4) ** -0.5, 0.25, ((1, 2),))
    w_key = normal_values(seeds[2], (D, HEADS * KEY_DIM), (D // 4) ** -0.5, 0.25, ((1, 2),))
    w_value = normal_values(seeds[3], (D, HEADS * VALUE_DIM), D ** -0.5, 0.125, ((1, 2),))
    w_out = normal_values(seeds[4], (HEADS * VALUE_DIM, D), 0.3, 1.796875)
    return dict(tokens=tokens, w_query=w_query, w_key=w_key, w_value=w_value, w_out=w_out)


def taylor_features(rows):
    wide = rows.astype(jnp.float32)
    count = wide.shape[-1]
    outer = (wide[..., :, None] * wide[..., None, :]).reshape(wide.shape[:-1] + (count * count,))
    ones = jnp.ones(wide.shape[:-1] + (1,), jnp.float32)
    joined = jnp.concatenate([ones, wide / (count ** 0.25), outer / ((2.0 * count) ** 0.5)], axis=-1)
    return joined.astype(jnp.bfloat16)


def reference(tokens, w_query, w_key, w_value, w_out):
    def span_step(carry, span_rows):
        prefix, zprefix = carry
        queries = jnp.dot(span_rows, w_query, preferred_element_type=jnp.float32).astype(jnp.bfloat16).reshape(TOK_DEV, HEADS, KEY_DIM)
        key_rows = jnp.dot(span_rows, w_key, preferred_element_type=jnp.float32).astype(jnp.bfloat16).reshape(TOK_DEV, HEADS, KEY_DIM)
        val_rows = jnp.dot(span_rows, w_value, preferred_element_type=jnp.float32).astype(jnp.bfloat16).reshape(TOK_DEV, HEADS, VALUE_DIM)
        query_feat = taylor_features(queries)
        key_feat = taylor_features(key_rows)
        state = jnp.einsum('thf,thv->hfv', key_feat.astype(jnp.float32), val_rows.astype(jnp.float32), precision=lax.Precision.HIGHEST)
        norm_sum = jnp.sum(key_feat.astype(jnp.float32), axis=0)
        prefix_low = prefix.astype(jnp.bfloat16)
        numer_pre = jnp.einsum('thf,hfv->thv', query_feat.astype(jnp.float32), prefix_low.astype(jnp.float32), precision=lax.Precision.HIGHEST)
        denom_pre = jnp.einsum('thf,hf->th', query_feat.astype(jnp.float32), zprefix, precision=lax.Precision.HIGHEST)
        block = min(512, TOK_DEV)
        outputs = []
        for index in range(TOK_DEV // block):
            low = index * block
            high = low + block
            q_block = queries[low:high].astype(jnp.float32)
            k_block = key_rows[:high].astype(jnp.float32)
            scores = jnp.einsum('qhd,khd->hqk', q_block, k_block) / (KEY_DIM ** 0.5)
            taylor = 1.0 + scores + 0.5 * scores * scores
            row_ids = low + jnp.arange(block, dtype=jnp.int32)[:, None]
            col_ids = jnp.arange(high, dtype=jnp.int32)[None, :]
            taylor = jnp.where((col_ids <= row_ids)[None], taylor, 0.0)
            denom = denom_pre[low:high] + jnp.transpose(jnp.sum(taylor, axis=-1))
            taylor_low = taylor.astype(jnp.bfloat16)
            numer_in = jnp.einsum('hqk,khv->qhv', taylor_low.astype(jnp.float32), val_rows[:high].astype(jnp.float32))
            numer = numer_pre[low:high] + numer_in
            outputs.append((numer / denom[..., None]).astype(jnp.bfloat16))
        attended = jnp.concatenate(outputs, axis=0).reshape(TOK_DEV, HEADS * VALUE_DIM)
        mixed_rows = jnp.dot(attended, w_out, preferred_element_type=jnp.float32).astype(jnp.bfloat16)
        return (prefix + state, zprefix + norm_sum), mixed_rows

    init = (jnp.zeros((HEADS, FEATURES, VALUE_DIM), jnp.float32), jnp.zeros((HEADS, FEATURES), jnp.float32))
    spans = tokens.reshape(N_SEQ, TOK_DEV, D)
    final, mixed = lax.scan(span_step, init, spans)
    return mixed.reshape(TOKENS, D)
```

```python
import functools

import jax
import jax.numpy as jnp
from jax import lax
from jax.experimental import pallas as pl
from jax.experimental.pallas import tpu as pltpu
from jax.sharding import PartitionSpec as P

KEY_DIM = 16
VALUE_DIM = 128
ROWS = 160
PAIR = 2
MESH = pl.DeviceIdType.MESH
F32 = jnp.float32
BF16 = jnp.bfloat16


def features(u, tail_one, square):
    n = u.shape[1]
    twice = jnp.concatenate([u, u], axis=0)
    parts = [u, u * u * square]
    for d in range(1, KEY_DIM // 2):
        parts.append(u * twice[d : d + KEY_DIM])
    half = KEY_DIM // 2
    parts.append(u[:half] * u[half:])
    row = lax.broadcasted_iota(jnp.int32, (8, n), 0)
    parts.append(jnp.where(row == 0, tail_one, 0.0))
    return jnp.concatenate(parts, axis=0)


def pack_norm(total):
    state, norm = total[:, :VALUE_DIM], total[:, VALUE_DIM:]
    top = norm[:VALUE_DIM]
    rest = norm[VALUE_DIM:]

    def diagonal(block):
        r = lax.broadcasted_iota(jnp.int32, block.shape, 0)
        l = lax.broadcasted_iota(jnp.int32, block.shape, 1)
        return jnp.sum(jnp.where(r == l, block, 0.0), axis=0, keepdims=True)

    first, second = diagonal(top), diagonal(rest)
    r = lax.broadcasted_iota(jnp.int32, (8, VALUE_DIM), 0)
    tail = jnp.where(r == 0, state[ROWS - 8 :], jnp.where(r == 1, first, jnp.where(r == 2, second, 0.0)))
    return jnp.concatenate([state[: ROWS - 8], tail], axis=0)


def unpack_norm(packed):
    tail = packed[ROWS - 8 :]

    def column(row, height):
        r = lax.broadcasted_iota(jnp.int32, (height, VALUE_DIM), 0)
        l = lax.broadcasted_iota(jnp.int32, (height, VALUE_DIM), 1)
        return jnp.sum(jnp.where(r == l, row, 0.0), axis=1, keepdims=True)

    return jnp.concatenate([column(tail[1:2], VALUE_DIM), column(tail[2:3], ROWS - VALUE_DIM)], axis=0)


def kernel(
    n_seq, chunk,
    tok_hbm, wq_hbm, wk_hbm, wv_hbm, wo_hbm, out_ref,
    tok, wqk, wv, wo, vals, qs, qt, kt, local, inner, qfeat, att,
    own, base, plane, send_x, recv_x, send_y, recv_y, send_z, recv_z,
    load_sem, x_ss, x_rs, y_ss, y_rs, z_ss, z_rs, a_ss, a_rs,
):
    rows, width = tok.shape
    heads = vals.shape[0]
    groups = heads // PAIR
    chunks = rows // chunk
    cols_here = wo.shape[1]
    chain = n_seq // 4
    seq = lax.axis_index("seq")
    core = lax.axis_index("head")
    x = lax.rem(seq, 2)
    y = lax.rem(seq // 2, 2)
    z = seq // 4
    x_peer = seq + 1 - 2 * x
    y_peer = seq + 2 - 4 * y
    up = lax.rem(seq + 4, n_seq)
    down = lax.rem(seq + n_seq - 4, n_seq)

    load_qk = [
        pltpu.make_async_copy(wq_hbm, wqk.at[:, pl.ds(0, 128)], load_sem.at[0]),
        pltpu.make_async_copy(wk_hbm, wqk.at[:, pl.ds(128, 128)], load_sem.at[1]),
        pltpu.make_async_copy(tok_hbm, tok, load_sem.at[2]),
    ]
    load_v = pltpu.make_async_copy(wv_hbm, wv, load_sem.at[3])
    load_o = pltpu.make_async_copy(
        wo_hbm.at[:, pl.ds(pl.multiple_of(core * cols_here, 128), cols_here)], wo, load_sem.at[4]
    )
    for c in load_qk:
        c.start()
    load_v.start()

    barrier = pltpu.get_barrier_semaphore()
    for peer in (x_peer, y_peer, up, down):
        pl.semaphore_signal(barrier, inc=1, device_id=(peer, core), device_id_type=MESH)
    pl.semaphore_signal(barrier, inc=1, device_id=(seq, 1 - core), device_id_type=MESH)
    pl.semaphore_wait(barrier, 5)

    def copy_x(g):
        return pltpu.make_async_remote_copy(
            src_ref=send_x.at[g], dst_ref=recv_x.at[g], send_sem=x_ss.at[g], recv_sem=x_rs.at[g],
            device_id=(x_peer, core), device_id_type=MESH)

    def copy_y(g):
        return pltpu.make_async_remote_copy(
            src_ref=send_y.at[g], dst_ref=recv_y.at[g], send_sem=y_ss.at[g], recv_sem=y_rs.at[g],
            device_id=(y_peer, core), device_id_type=MESH)

    def copy_z(g):
        return pltpu.make_async_remote_copy(
            src_ref=send_z.at[g], dst_ref=recv_z.at[g], send_sem=z_ss.at[g], recv_sem=z_rs.at[g],
            device_id=(up, core), device_id_type=MESH)

    def copy_a(g):
        at = pl.ds(pl.multiple_of(core * (heads * VALUE_DIM) + g * (PAIR * VALUE_DIM), 128), PAIR * VALUE_DIM)
        return pltpu.make_async_remote_copy(
            src_ref=att.at[:, at], dst_ref=att.at[:, at], send_sem=a_ss.at[g], recv_sem=a_rs.at[g],
            device_id=(seq, 1 - core), device_id_type=MESH)

    def pump(t):
        gx, gy, gz = t - 1, t - 2, t - 2 - z

        @pl.when((gx >= 0) & (gx < groups))
        def _():
            copy_x(gx).wait_recv()
            other = recv_x[gx].astype(F32)
            both = own[gx] + other
            send_y[gx] = both.astype(BF16)
            copy_y(gx).start()
            plane[gx] = both
            base[gx] = jnp.where(x == 1, other, 0.0)

        @pl.when((gy >= 0) & (gy < groups))
        def _():
            copy_y(gy).wait_recv()
            other = recv_y[gy].astype(F32)
            plane[gy] = plane[gy] + other
            base[gy] = base[gy] + jnp.where(y == 1, other, 0.0)

        @pl.when((gz >= 0) & (gz < groups))
        def _():
            @pl.when(z > 0)
            def _():
                copy_z(gz).wait_recv()
                earlier = recv_z[gz].astype(F32)
                base[gz] = base[gz] + earlier
                plane[gz] = plane[gz] + earlier

            @pl.when(z < chain - 1)
            def _():
                send_z[gz] = plane[gz].astype(BF16)
                copy_z(gz).start()

    for c in load_qk:
        c.wait()
    load_o.start()
    qk = jnp.dot(tok[...], wqk[...], preferred_element_type=F32).astype(BF16).astype(F32)
    q = qk[:, :128] * 0.25
    qs[...] = q.astype(BF16)
    qt[...] = q.T
    kt[...] = qk[:, 128:].T
    load_v.wait()

    def head_rows(h):
        return pl.ds(pl.multiple_of(h * KEY_DIM, KEY_DIM), KEY_DIM)

    def group_step(g, _):
        at = pl.ds(pl.multiple_of(g * (PAIR * VALUE_DIM), 128), PAIR * VALUE_DIM)
        v = jnp.dot(tok[...], wv[:, at], preferred_element_type=F32).astype(BF16)
        for i in range(PAIR):
            vals[g * PAIR + i] = v[:, i * VALUE_DIM : (i + 1) * VALUE_DIM]
        ones = jnp.ones((chunk, VALUE_DIM), BF16)
        for i in range(PAIR):
            h = g * PAIR + i
            total = jnp.zeros((ROWS, 2 * VALUE_DIM), F32)
            for c in range(chunks):
                local[h, c] = total
                feat = features(kt[head_rows(h), pl.ds(c * chunk, chunk)], 1.0, 1.0).astype(BF16)
                wide = jnp.concatenate([vals[h, pl.ds(c * chunk, chunk)], ones], axis=1)
                total = total + jnp.dot(feat, wide, preferred_element_type=F32)
            packed = pack_norm(total)
            own[g, i] = packed
            send_x[g, i] = packed.astype(BF16)
        copy_x(g).start()
        pump(g)
        return 0

    lax.fori_loop(0, groups, group_step, 0)

    def inner_step(h, _):
        row_head = lax.broadcasted_iota(jnp.int32, (128, chunk), 0) // KEY_DIM
        r = lax.broadcasted_iota(jnp.int32, (chunk, chunk), 0)
        l = lax.broadcasted_iota(jnp.int32, (chunk, chunk), 1)
        ones = jnp.ones((chunk, VALUE_DIM), BF16)
        for c in range(chunks):
            span = pl.ds(c * chunk, chunk)
            k_own = jnp.where(row_head == h, kt[:, span], 0.0).astype(BF16)
            s = jnp.dot(qs[span], k_own, preferred_element_type=F32)
            s1 = s + 1.0
            taylor = jnp.where(l <= r, 0.5 * (s1 * s1) + 0.5, 0.0).astype(BF16)
            wide = jnp.concatenate([vals[h, span], ones], axis=1)
            inner[h, span] = jnp.dot(taylor, wide, preferred_element_type=F32)
            feat = features(qt[head_rows(h), span], 1.0, 0.5)
            qfeat[h, span] = feat.T.astype(BF16)
        pump(groups + h)
        return 0

    lax.fori_loop(0, heads, inner_step, 0)

    def rest(t, _):
        pump(t)
        return 0

    lax.fori_loop(groups + heads, max(groups + heads, groups + chain + 2), rest, 0)

    def outer_step(g, _):
        for i in range(PAIR):
            h = g * PAIR + i
            packed = base[g, i]
            norm = jnp.broadcast_to(unpack_norm(packed), (ROWS, VALUE_DIM))
            entering = jnp.concatenate([packed, norm], axis=1)
            for c in range(chunks):
                span = pl.ds(c * chunk, chunk)
                prefix = (entering + local[h, c]).astype(BF16)
                total = inner[h, span] + jnp.dot(qfeat[h, span], prefix, preferred_element_type=F32)
                result = total[:, :VALUE_DIM] / total[:, VALUE_DIM:]
                at = pl.ds(pl.multiple_of(core * (heads * VALUE_DIM) + h * VALUE_DIM, 128), VALUE_DIM)
                att[span, at] = result.astype(BF16)
        copy_a(g).start()
        return 0

    lax.fori_loop(0, groups, outer_step, 0)
    load_o.wait()

    def await_peer(g, _):
        at = pl.ds(pl.multiple_of((1 - core) * (heads * VALUE_DIM) + g * (PAIR * VALUE_DIM), 128), PAIR * VALUE_DIM)
        pltpu.make_async_remote_copy(
            src_ref=att.at[:, at], dst_ref=att.at[:, at], send_sem=a_ss.at[g], recv_sem=a_rs.at[g],
            device_id=(seq, 1 - core), device_id_type=MESH).wait_recv()
        return 0

    lax.fori_loop(0, groups, await_peer, 0)

    def out_step(b, _):
        at = pl.ds(pl.multiple_of(b * 256, 128), 256)
        out_ref[:, at] = jnp.dot(att[...], wo[:, at], preferred_element_type=F32).astype(BF16)
        return 0

    lax.fori_loop(0, cols_here // 256, out_step, 0)

    def finish(g, _):
        copy_x(g).wait_send()
        copy_y(g).wait_send()
        copy_a(g).wait_send()

        @pl.when(z < chain - 1)
        def _():
            copy_z(g).wait_send()

        return 0

    lax.fori_loop(0, groups, finish, 0)


def per_device(tokens, w_query, w_key, w_value, w_out):
    n_seq = lax.axis_size("seq")
    rows, width = tokens.shape
    heads = w_query.shape[1] // KEY_DIM
    groups = heads // PAIR
    chunk = min(256, rows)
    cols = w_out.shape[1] // lax.axis_size("head")
    vm = pltpu.VMEM
    slot = (groups, PAIR, ROWS, VALUE_DIM)
    dma = pltpu.SemaphoreType.DMA
    return pl.pallas_call(
        functools.partial(kernel, n_seq, chunk),
        out_shape=jax.ShapeDtypeStruct((rows, cols), BF16),
        in_specs=[pl.BlockSpec(memory_space=pl.ANY)] * 5,
        out_specs=pl.BlockSpec(memory_space=pltpu.VMEM),
        scratch_shapes=[
            vm((rows, width), BF16),
            vm((width, 256), BF16),
            vm(w_value.shape, BF16),
            vm((w_out.shape[0], cols), BF16),
            vm((heads, rows, VALUE_DIM), BF16),
            vm((rows, 128), BF16),
            vm((128, rows), F32),
            vm((128, rows), F32),
            vm((heads, rows // chunk, ROWS, 2 * VALUE_DIM), F32),
            vm((heads, rows, 2 * VALUE_DIM), F32),
            vm((heads, rows, ROWS), BF16),
            vm((rows, w_out.shape[0]), BF16),
            vm(slot, F32), vm(slot, F32), vm(slot, F32),
            vm(slot, BF16), vm(slot, BF16), vm(slot, BF16), vm(slot, BF16), vm(slot, BF16), vm(slot, BF16),
            dma((5,)),
            dma((groups,)), dma((groups,)), dma((groups,)), dma((groups,)), dma((groups,)), dma((groups,)),
            dma((groups,)), dma((groups,)),
        ],
        compiler_params=pltpu.CompilerParams(
            collective_id=0, has_side_effects=True, vmem_limit_bytes=62 * 1024 * 1024
        ),
    )(tokens, w_query, w_key, w_value, w_out)


def solution(mesh):
    in_specs = (P("seq", None), P(None, "head"), P(None, "head"), P(None, "head"), P())
    return jax.shard_map(
        per_device, mesh=mesh, in_specs=in_specs, out_specs=P("seq", "head"), check_vma=False
    )
```

```python
import functools

import jax
import jax.numpy as jnp
from jax import lax
from jax.experimental import pallas as pl
from jax.experimental.pallas import tpu as pltpu
from jax.sharding import PartitionSpec as P

KEY_DIM = 16
VALUE_DIM = 128
ROWS = 160
PAIR = 2
LOADS = 2
MESH = pl.DeviceIdType.MESH
F32 = jnp.float32
BF16 = jnp.bfloat16


def features(u, tail_one, square):
    n = u.shape[1]
    twice = jnp.concatenate([u, u], axis=0)
    parts = [u, u * u * square]
    for d in range(1, KEY_DIM // 2):
        parts.append(u * twice[d : d + KEY_DIM])
    half = KEY_DIM // 2
    parts.append(u[:half] * u[half:])
    row = lax.broadcasted_iota(jnp.int32, (8, n), 0)
    parts.append(jnp.where(row == 0, tail_one, 0.0))
    return jnp.concatenate(parts, axis=0)


def pack_norm(total):
    state, norm = total[:, :VALUE_DIM], total[:, VALUE_DIM:]
    top = norm[:VALUE_DIM]
    rest = norm[VALUE_DIM:]

    def diagonal(block):
        r = lax.broadcasted_iota(jnp.int32, block.shape, 0)
        l = lax.broadcasted_iota(jnp.int32, block.shape, 1)
        return jnp.sum(jnp.where(r == l, block, 0.0), axis=0, keepdims=True)

    first, second = diagonal(top), diagonal(rest)
    r = lax.broadcasted_iota(jnp.int32, (8, VALUE_DIM), 0)
    tail = jnp.where(r == 0, state[ROWS - 8 :], jnp.where(r == 1, first, jnp.where(r == 2, second, 0.0)))
    return jnp.concatenate([state[: ROWS - 8], tail], axis=0)


def unpack_norm(packed):
    tail = packed[ROWS - 8 :]

    def column(row, height):
        r = lax.broadcasted_iota(jnp.int32, (height, VALUE_DIM), 0)
        l = lax.broadcasted_iota(jnp.int32, (height, VALUE_DIM), 1)
        return jnp.sum(jnp.where(r == l, row, 0.0), axis=1, keepdims=True)

    return jnp.concatenate([column(tail[1:2], VALUE_DIM), column(tail[2:3], ROWS - VALUE_DIM)], axis=0)


def kernel(
    n_seq, chunk,
    tok_hbm, wq_hbm, wk_hbm, wv_hbm, wo_hbm, out_ref,
    tok, wqk, wv, wo, vals, qs, qt, kt, local, inner, qfeat, att,
    own, base, plane, send_x, recv_x, send_y, recv_y, send_z, recv_z,
    acc, load_sem, tok_sem, v_sem, x_ss, x_rs, y_ss, y_rs, z_ss, z_rs, a_ss, a_rs,
):
    rows, width = tok.shape
    heads = vals.shape[0]
    groups = heads // PAIR
    chunks = rows // chunk
    cols_here = wo.shape[1]
    chain = n_seq // 4
    seq = lax.axis_index("seq")
    core = lax.axis_index("head")
    x = lax.rem(seq, 2)
    y = lax.rem(seq // 2, 2)
    z = seq // 4
    x_peer = seq + 1 - 2 * x
    y_peer = seq + 2 - 4 * y
    up = lax.rem(seq + 4, n_seq)
    down = lax.rem(seq + n_seq - 4, n_seq)

    half = rows // LOADS
    load_w = [
        pltpu.make_async_copy(wk_hbm, wqk.at[:, pl.ds(128, 128)], load_sem.at[1]),
        pltpu.make_async_copy(wq_hbm, wqk.at[:, pl.ds(0, 128)], load_sem.at[0]),
    ]
    load_t = [
        pltpu.make_async_copy(tok_hbm.at[pl.ds(i * half, half)], tok.at[pl.ds(i * half, half)], tok_sem.at[i])
        for i in range(LOADS)
    ]
    load_o = pltpu.make_async_copy(
        wo_hbm.at[:, pl.ds(pl.multiple_of(core * cols_here, 128), cols_here)], wo, load_sem.at[2]
    )

    def load_v(g):
        at = pl.ds(pl.multiple_of(g * (PAIR * VALUE_DIM), 128), PAIR * VALUE_DIM)
        return pltpu.make_async_copy(wv_hbm.at[:, at], wv.at[:, at], v_sem.at[g])

    for c in load_w:
        c.start()
    for c in load_t:
        c.start()
    for g in range(groups):
        load_v(g).start()

    barrier = pltpu.get_barrier_semaphore()
    for peer in (x_peer, y_peer, up, down):
        pl.semaphore_signal(barrier, inc=1, device_id=(peer, core), device_id_type=MESH)
    pl.semaphore_signal(barrier, inc=1, device_id=(seq, 1 - core), device_id_type=MESH)

    def copy_x(g):
        return pltpu.make_async_remote_copy(
            src_ref=send_x.at[g], dst_ref=recv_x.at[g], send_sem=x_ss.at[g], recv_sem=x_rs.at[g],
            device_id=(x_peer, core), device_id_type=MESH)

    def copy_y(g):
        return pltpu.make_async_remote_copy(
            src_ref=send_y.at[g], dst_ref=recv_y.at[g], send_sem=y_ss.at[g], recv_sem=y_rs.at[g],
            device_id=(y_peer, core), device_id_type=MESH)

    def copy_z(g):
        return pltpu.make_async_remote_copy(
            src_ref=send_z.at[g], dst_ref=recv_z.at[g], send_sem=z_ss.at[g], recv_sem=z_rs.at[g],
            device_id=(up, core), device_id_type=MESH)

    def copy_a(g):
        at = pl.ds(pl.multiple_of(core * (heads * VALUE_DIM) + g * (PAIR * VALUE_DIM), 128), PAIR * VALUE_DIM)
        return pltpu.make_async_remote_copy(
            src_ref=att.at[:, at], dst_ref=att.at[:, at], send_sem=a_ss.at[g], recv_sem=a_rs.at[g],
            device_id=(seq, 1 - core), device_id_type=MESH)

    def pump(t):
        gx, gy, gz = t - 3, t - 6, t - 6 - 3 * z

        @pl.when((gx >= 0) & (gx < heads))
        def _():
            copy_x(gx).wait_recv()
            other = recv_x[gx].astype(F32)
            both = own[gx] + other
            send_y[gx] = both.astype(BF16)
            copy_y(gx).start()
            plane[gx] = both
            base[gx] = jnp.where(x == 1, other, 0.0)

        @pl.when((gy >= 0) & (gy < heads))
        def _():
            copy_y(gy).wait_recv()
            other = recv_y[gy].astype(F32)
            plane[gy] = plane[gy] + other
            base[gy] = base[gy] + jnp.where(y == 1, other, 0.0)

        @pl.when((gz >= 0) & (gz < heads) & (z < chain - 1))
        def _():
            @pl.when(z > 0)
            def _():
                copy_z(gz).wait_recv()
                earlier = recv_z[gz].astype(F32)
                base[gz] = base[gz] + earlier
                plane[gz] = plane[gz] + earlier

            send_z[gz] = plane[gz].astype(BF16)
            copy_z(gz).start()

    for c in load_w:
        c.wait()
    for i in range(LOADS):
        load_t[i].wait()
        part = pl.ds(i * half, half)
        qk = jnp.dot(tok[part], wqk[...], preferred_element_type=F32).astype(BF16).astype(F32)
        q = qk[:, :128] * 0.25
        qs[part] = q.astype(BF16)
        qt[:, part] = q.T
        kt[:, part] = qk[:, 128:].T
    load_o.start()
    pl.semaphore_wait(barrier, 5)

    def head_rows(h):
        return pl.ds(pl.multiple_of(h * KEY_DIM, KEY_DIM), KEY_DIM)

    def group_step(g, _):
        at = pl.ds(pl.multiple_of(g * (PAIR * VALUE_DIM), 128), PAIR * VALUE_DIM)
        load_v(g).wait()
        v = jnp.dot(tok[...], wv[:, at], preferred_element_type=F32).astype(BF16)
        for i in range(PAIR):
            vals[g * PAIR + i] = v[:, i * VALUE_DIM : (i + 1) * VALUE_DIM]
        ones = jnp.ones((chunk, VALUE_DIM), BF16)
        for i in range(PAIR):
            h = g * PAIR + i
            total = jnp.zeros((ROWS, 2 * VALUE_DIM), F32)
            for c in range(chunks):
                local[h, c] = total
                feat = features(kt[head_rows(h), pl.ds(c * chunk, chunk)], 1.0, 1.0).astype(BF16)
                wide = jnp.concatenate([vals[h, pl.ds(c * chunk, chunk)], ones], axis=1)
                total = total + jnp.dot(feat, wide, preferred_element_type=F32)
            packed = pack_norm(total)
            own[h] = packed
            send_x[h] = packed.astype(BF16)
            copy_x(h).start()
            pump(h)
        return 0

    lax.fori_loop(0, groups, group_step, 0)

    def inner_head(h):
        row_head = lax.broadcasted_iota(jnp.int32, (128, chunk), 0) // KEY_DIM
        r = lax.broadcasted_iota(jnp.int32, (chunk, chunk), 0)
        l = lax.broadcasted_iota(jnp.int32, (chunk, chunk), 1)
        ones = jnp.ones((chunk, VALUE_DIM), BF16)
        for c in range(chunks):
            span = pl.ds(c * chunk, chunk)
            k_own = jnp.where(row_head == h, kt[:, span], 0.0).astype(BF16)
            s = jnp.dot(qs[span], k_own, preferred_element_type=F32)
            s1 = s + 1.0
            taylor = jnp.where(l <= r, 0.5 * (s1 * s1) + 0.5, 0.0).astype(BF16)
            wide = jnp.concatenate([vals[h, span], ones], axis=1)
            inner[h, span] = jnp.dot(taylor, wide, preferred_element_type=F32)
            feat = features(qt[head_rows(h), span], 1.0, 0.5)
            qfeat[h, span] = feat.T.astype(BF16)

    def inner_step(g, _):
        for i in range(PAIR):
            inner_head(g * PAIR + i)
        pump(heads + g)
        return 0

    lax.fori_loop(0, groups, inner_step, 0)

    first = heads + groups

    def pumped(g):
        return jnp.maximum(first + 1 + g, PAIR * (g + 1) + 6 + 3 * (chain - 2))

    def rest(t, _):
        pump(t)
        return 0

    def outer_step(g):
        lax.fori_loop(jnp.where(g == 0, first, pumped(g - 1)), pumped(g), rest, 0)
        for i in range(PAIR):
            h = g * PAIR + i

            @pl.when(z == chain - 1)
            def _():
                copy_z(h).wait_recv()
                base[h] = base[h] + recv_z[h].astype(F32)

            packed = base[h]
            norm = jnp.broadcast_to(unpack_norm(packed), (ROWS, VALUE_DIM))
            entering = jnp.concatenate([packed, norm], axis=1)
            for c in range(chunks):
                span = pl.ds(c * chunk, chunk)
                prefix = (entering + local[h, c]).astype(BF16)
                total = inner[h, span] + jnp.dot(qfeat[h, span], prefix, preferred_element_type=F32)
                result = total[:, :VALUE_DIM] / total[:, VALUE_DIM:]
                at = pl.ds(pl.multiple_of(core * (heads * VALUE_DIM) + h * VALUE_DIM, 128), VALUE_DIM)
                att[span, at] = result.astype(BF16)
        copy_a(g).start()

    own_at, peer_at = core * (heads * VALUE_DIM), (1 - core) * (heads * VALUE_DIM)
    step = PAIR * VALUE_DIM

    def out_step(g, begin, end):
        here = pl.ds(pl.multiple_of(own_at + g * step, 128), step)
        there = pl.ds(pl.multiple_of(peer_at + g * step, 128), step)
        pltpu.make_async_remote_copy(
            src_ref=att.at[:, there], dst_ref=att.at[:, there], send_sem=a_ss.at[g], recv_sem=a_rs.at[g],
            device_id=(seq, 1 - core), device_id_type=MESH).wait_recv()

        def block(b, _):
            at = pl.ds(pl.multiple_of(b * 256, 128), 256)
            both = jnp.concatenate([att[:, here], att[:, there]], axis=1)
            part = jnp.dot(both, jnp.concatenate([wo[here, at], wo[there, at]], axis=0), preferred_element_type=F32)
            if not begin:
                part = part + acc[:, at]
            if end:
                out_ref[:, at] = part.astype(BF16)
            else:
                acc[:, at] = part
            return 0

        lax.fori_loop(0, cols_here // 256, block, 0)

    outer_step(0)
    load_o.wait()
    outer_step(1)
    out_step(0, True, False)

    def later(g, _):
        outer_step(g)
        out_step(g - 1, False, False)
        return 0

    lax.fori_loop(2, groups, later, 0)
    out_step(groups - 1, False, True)

    def finish(g, _):
        copy_a(g).wait_send()
        for i in range(PAIR):
            h = g * PAIR + i
            copy_x(h).wait_send()
            copy_y(h).wait_send()

            @pl.when(z < chain - 1)
            def _():
                copy_z(h).wait_send()

        return 0

    lax.fori_loop(0, groups, finish, 0)


def per_device(tokens, w_query, w_key, w_value, w_out):
    n_seq = lax.axis_size("seq")
    rows, width = tokens.shape
    heads = w_query.shape[1] // KEY_DIM
    groups = heads // PAIR
    chunk = min(256, rows)
    cols = w_out.shape[1] // lax.axis_size("head")
    vm = pltpu.VMEM
    slot = (heads, ROWS, VALUE_DIM)
    dma = pltpu.SemaphoreType.DMA
    return pl.pallas_call(
        functools.partial(kernel, n_seq, chunk),
        out_shape=jax.ShapeDtypeStruct((rows, cols), BF16),
        in_specs=[pl.BlockSpec(memory_space=pl.ANY)] * 5,
        out_specs=pl.BlockSpec(memory_space=pltpu.VMEM),
        scratch_shapes=[
            vm((rows, width), BF16),
            vm((width, 256), BF16),
            vm(w_value.shape, BF16),
            vm((w_out.shape[0], cols), BF16),
            vm((heads, rows, VALUE_DIM), BF16),
            vm((rows, 128), BF16),
            vm((128, rows), F32),
            vm((128, rows), F32),
            vm((heads, rows // chunk, ROWS, 2 * VALUE_DIM), F32),
            vm((heads, rows, 2 * VALUE_DIM), F32),
            vm((heads, rows, ROWS), BF16),
            vm((rows, w_out.shape[0]), BF16),
            vm(slot, F32), vm(slot, F32), vm(slot, F32),
            vm(slot, BF16), vm(slot, BF16), vm(slot, BF16), vm(slot, BF16), vm(slot, BF16), vm(slot, BF16),
            vm((rows, cols), F32),
            dma((3,)), dma((LOADS,)), dma((groups,)),
            dma((heads,)), dma((heads,)), dma((heads,)), dma((heads,)), dma((heads,)), dma((heads,)),
            dma((groups,)), dma((groups,)),
        ],
        compiler_params=pltpu.CompilerParams(
            collective_id=0, has_side_effects=True, vmem_limit_bytes=50 * 1024 * 1024
        ),
    )(tokens, w_query, w_key, w_value, w_out)


def solution(mesh):
    in_specs = (P("seq", None), P(None, "head"), P(None, "head"), P(None, "head"), P())
    return jax.shard_map(
        per_device, mesh=mesh, in_specs=in_specs, out_specs=P("seq", "head"), check_vma=False
    )
```

```python
import functools

import jax
import jax.numpy as jnp
from jax import lax
from jax.experimental import pallas as pl
from jax.experimental.pallas import tpu as pltpu
from jax.sharding import PartitionSpec as P

KEY_DIM = 16
VALUE_DIM = 128
ROWS = 160
PAIR = 2
LOADS = 4
MESH = pl.DeviceIdType.MESH
F32 = jnp.float32
BF16 = jnp.bfloat16


def features(u, tail_one, square):
    n = u.shape[1]
    twice = jnp.concatenate([u, u], axis=0)
    parts = [u, u * u * square]
    for d in range(1, KEY_DIM // 2):
        parts.append(u * twice[d : d + KEY_DIM])
    half = KEY_DIM // 2
    parts.append(u[:half] * u[half:])
    row = lax.broadcasted_iota(jnp.int32, (8, n), 0)
    parts.append(jnp.where(row == 0, tail_one, 0.0))
    return jnp.concatenate(parts, axis=0)


def pack_norm(total):
    state, norm = total[:, :VALUE_DIM], total[:, VALUE_DIM:]
    top = norm[:VALUE_DIM]
    rest = norm[VALUE_DIM:]

    def diagonal(block):
        r = lax.broadcasted_iota(jnp.int32, block.shape, 0)
        l = lax.broadcasted_iota(jnp.int32, block.shape, 1)
        return jnp.sum(jnp.where(r == l, block, 0.0), axis=0, keepdims=True)

    first, second = diagonal(top), diagonal(rest)
    r = lax.broadcasted_iota(jnp.int32, (8, VALUE_DIM), 0)
    tail = jnp.where(r == 0, state[ROWS - 8 :], jnp.where(r == 1, first, jnp.where(r == 2, second, 0.0)))
    return jnp.concatenate([state[: ROWS - 8], tail], axis=0)


def unpack_norm(packed):
    tail = packed[ROWS - 8 :]

    def column(row, height):
        r = lax.broadcasted_iota(jnp.int32, (height, VALUE_DIM), 0)
        l = lax.broadcasted_iota(jnp.int32, (height, VALUE_DIM), 1)
        return jnp.sum(jnp.where(r == l, row, 0.0), axis=1, keepdims=True)

    return jnp.concatenate([column(tail[1:2], VALUE_DIM), column(tail[2:3], ROWS - VALUE_DIM)], axis=0)


def kernel(
    n_seq, chunk,
    tok_hbm, wq_hbm, wk_hbm, wv_hbm, wo_hbm, out_ref,
    tok, wqk, wv, wo, vals, qs, qt, kt, local, inner, qfeat, att,
    own, base, plane, send_x, recv_x, send_y, recv_y, send_z, recv_z,
    acc, load_sem, tok_sem, v_sem, x_ss, x_rs, y_ss, y_rs, z_ss, z_rs, a_ss, a_rs,
):
    rows, width = tok.shape
    heads = vals.shape[0]
    groups = heads // PAIR
    chunks = rows // chunk
    cols_here = wo.shape[1]
    chain = n_seq // 4
    seq = lax.axis_index("seq")
    core = lax.axis_index("head")
    x = lax.rem(seq, 2)
    y = lax.rem(seq // 2, 2)
    z = seq // 4
    x_peer = seq + 1 - 2 * x
    y_peer = seq + 2 - 4 * y
    up = lax.rem(seq + 4, n_seq)
    down = lax.rem(seq + n_seq - 4, n_seq)

    half = rows // LOADS
    load_w = [
        pltpu.make_async_copy(wk_hbm, wqk.at[:, pl.ds(128, 128)], load_sem.at[1]),
        pltpu.make_async_copy(wq_hbm, wqk.at[:, pl.ds(0, 128)], load_sem.at[0]),
    ]
    load_t = [
        pltpu.make_async_copy(tok_hbm.at[pl.ds(i * half, half)], tok.at[pl.ds(i * half, half)], tok_sem.at[i])
        for i in range(LOADS)
    ]
    load_o = pltpu.make_async_copy(
        wo_hbm.at[:, pl.ds(pl.multiple_of(core * cols_here, 128), cols_here)], wo, load_sem.at[2]
    )

    def load_v(g):
        at = pl.ds(pl.multiple_of(g * (PAIR * VALUE_DIM), 128), PAIR * VALUE_DIM)
        return pltpu.make_async_copy(wv_hbm.at[:, at], wv.at[:, at], v_sem.at[g])

    for c in load_w:
        c.start()
    for c in load_t:
        c.start()
    for g in range(groups):
        load_v(g).start()

    barrier = pltpu.get_barrier_semaphore()
    for peer in (x_peer, y_peer, up, down):
        pl.semaphore_signal(barrier, inc=1, device_id=(peer, core), device_id_type=MESH)
    pl.semaphore_signal(barrier, inc=1, device_id=(seq, 1 - core), device_id_type=MESH)

    def copy_x(g):
        return pltpu.make_async_remote_copy(
            src_ref=send_x.at[g], dst_ref=recv_x.at[g], send_sem=x_ss.at[g], recv_sem=x_rs.at[g],
            device_id=(x_peer, core), device_id_type=MESH)

    def copy_y(g):
        return pltpu.make_async_remote_copy(
            src_ref=send_y.at[g], dst_ref=recv_y.at[g], send_sem=y_ss.at[g], recv_sem=y_rs.at[g],
            device_id=(y_peer, core), device_id_type=MESH)

    def copy_z(g):
        return pltpu.make_async_remote_copy(
            src_ref=send_z.at[g], dst_ref=recv_z.at[g], send_sem=z_ss.at[g], recv_sem=z_rs.at[g],
            device_id=(up, core), device_id_type=MESH)

    def copy_a(g):
        at = pl.ds(pl.multiple_of(core * (heads * VALUE_DIM) + g * (PAIR * VALUE_DIM), 128), PAIR * VALUE_DIM)
        return pltpu.make_async_remote_copy(
            src_ref=att.at[:, at], dst_ref=att.at[:, at], send_sem=a_ss.at[g], recv_sem=a_rs.at[g],
            device_id=(seq, 1 - core), device_id_type=MESH)

    def pump(t):
        gx, gy, gz = t - 3, t - 6, t - 6 - 3 * z

        @pl.when((gx >= 0) & (gx < heads))
        def _():
            copy_x(gx).wait_recv()
            other = recv_x[gx].astype(F32)
            both = own[gx] + other
            send_y[gx] = both.astype(BF16)
            copy_y(gx).start()
            plane[gx] = both
            base[gx] = jnp.where(x == 1, other, 0.0)

        @pl.when((gy >= 0) & (gy < heads))
        def _():
            copy_y(gy).wait_recv()
            other = recv_y[gy].astype(F32)
            plane[gy] = plane[gy] + other
            base[gy] = base[gy] + jnp.where(y == 1, other, 0.0)

        @pl.when((gz >= 0) & (gz < heads) & (z < chain - 1))
        def _():
            @pl.when(z > 0)
            def _():
                copy_z(gz).wait_recv()
                earlier = recv_z[gz].astype(F32)
                base[gz] = base[gz] + earlier
                plane[gz] = plane[gz] + earlier

            send_z[gz] = plane[gz].astype(BF16)
            copy_z(gz).start()

    for c in load_w:
        c.wait()
    for i in range(LOADS):
        load_t[i].wait()
        part = pl.ds(i * half, half)
        qk = jnp.dot(tok[part], wqk[...], preferred_element_type=F32).astype(BF16).astype(F32)
        q = qk[:, :128] * 0.25
        qs[part] = q.astype(BF16)
        qt[:, part] = q.T
        kt[:, part] = qk[:, 128:].T
    load_o.start()
    pl.semaphore_wait(barrier, 5)

    def head_rows(h):
        return pl.ds(pl.multiple_of(h * KEY_DIM, KEY_DIM), KEY_DIM)

    def group_step(g, _):
        at = pl.ds(pl.multiple_of(g * (PAIR * VALUE_DIM), 128), PAIR * VALUE_DIM)
        load_v(g).wait()
        v = jnp.dot(tok[...], wv[:, at], preferred_element_type=F32).astype(BF16)
        for i in range(PAIR):
            vals[g * PAIR + i] = v[:, i * VALUE_DIM : (i + 1) * VALUE_DIM]
        ones = jnp.ones((chunk, VALUE_DIM), BF16)
        for i in range(PAIR):
            h = g * PAIR + i
            total = jnp.zeros((ROWS, 2 * VALUE_DIM), F32)
            for c in range(chunks):
                local[h, c] = total
                feat = features(kt[head_rows(h), pl.ds(c * chunk, chunk)], 1.0, 1.0).astype(BF16)
                wide = jnp.concatenate([vals[h, pl.ds(c * chunk, chunk)], ones], axis=1)
                total = total + jnp.dot(feat, wide, preferred_element_type=F32)
            packed = pack_norm(total)
            own[h] = packed
            send_x[h] = packed.astype(BF16)
            copy_x(h).start()
            pump(h)
        return 0

    lax.fori_loop(0, groups, group_step, 0)

    def inner_head(h):
        row_head = lax.broadcasted_iota(jnp.int32, (128, chunk), 0) // KEY_DIM
        r = lax.broadcasted_iota(jnp.int32, (chunk, chunk), 0)
        l = lax.broadcasted_iota(jnp.int32, (chunk, chunk), 1)
        ones = jnp.ones((chunk, VALUE_DIM), BF16)
        for c in range(chunks):
            span = pl.ds(c * chunk, chunk)
            k_own = jnp.where(row_head == h, kt[:, span], 0.0).astype(BF16)
            s = jnp.dot(qs[span], k_own, preferred_element_type=F32)
            s1 = s + 1.0
            taylor = jnp.where(l <= r, 0.5 * (s1 * s1) + 0.5, 0.0).astype(BF16)
            wide = jnp.concatenate([vals[h, span], ones], axis=1)
            inner[h, span] = jnp.dot(taylor, wide, preferred_element_type=F32)
            feat = features(qt[head_rows(h), span], 1.0, 0.5)
            qfeat[h, span] = feat.T.astype(BF16)

    def inner_step(g, _):
        for i in range(PAIR):
            inner_head(g * PAIR + i)
        pump(heads + g)
        return 0

    lax.fori_loop(0, groups, inner_step, 0)

    first = heads + groups

    def pumped(g):
        return jnp.maximum(first + 1 + g, PAIR * (g + 1) + 6 + 3 * (chain - 2))

    def rest(t, _):
        pump(t)
        return 0

    def outer_step(g):
        lax.fori_loop(jnp.where(g == 0, first, pumped(g - 1)), pumped(g), rest, 0)
        for i in range(PAIR):
            h = g * PAIR + i

            @pl.when(z == chain - 1)
            def _():
                copy_z(h).wait_recv()
                base[h] = base[h] + recv_z[h].astype(F32)

            packed = base[h]
            norm = jnp.broadcast_to(unpack_norm(packed), (ROWS, VALUE_DIM))
            entering = jnp.concatenate([packed, norm], axis=1)
            for c in range(chunks):
                span = pl.ds(c * chunk, chunk)
                prefix = (entering + local[h, c]).astype(BF16)
                total = inner[h, span] + jnp.dot(qfeat[h, span], prefix, preferred_element_type=F32)
                result = total[:, :VALUE_DIM] / total[:, VALUE_DIM:]
                at = pl.ds(pl.multiple_of(core * (heads * VALUE_DIM) + h * VALUE_DIM, 128), VALUE_DIM)
                att[span, at] = result.astype(BF16)
        copy_a(g).start()

    own_at, peer_at = core * (heads * VALUE_DIM), (1 - core) * (heads * VALUE_DIM)
    step = PAIR * VALUE_DIM

    def out_step(g, begin, end):
        here = pl.ds(pl.multiple_of(own_at + g * step, 128), step)
        there = pl.ds(pl.multiple_of(peer_at + g * step, 128), step)
        pltpu.make_async_remote_copy(
            src_ref=att.at[:, there], dst_ref=att.at[:, there], send_sem=a_ss.at[g], recv_sem=a_rs.at[g],
            device_id=(seq, 1 - core), device_id_type=MESH).wait_recv()

        def block(b, _):
            at = pl.ds(pl.multiple_of(b * 256, 128), 256)
            both = jnp.concatenate([att[:, here], att[:, there]], axis=1)
            part = jnp.dot(both, jnp.concatenate([wo[here, at], wo[there, at]], axis=0), preferred_element_type=F32)
            if not begin:
                part = part + acc[:, at]
            if end:
                out_ref[:, at] = part.astype(BF16)
            else:
                acc[:, at] = part
            return 0

        lax.fori_loop(0, cols_here // 256, block, 0)

    outer_step(0)
    load_o.wait()
    outer_step(1)
    out_step(0, True, False)

    def later(g, _):
        outer_step(g)
        out_step(g - 1, False, False)
        return 0

    lax.fori_loop(2, groups, later, 0)
    out_step(groups - 1, False, True)

    def finish(g, _):
        copy_a(g).wait_send()
        for i in range(PAIR):
            h = g * PAIR + i
            copy_x(h).wait_send()
            copy_y(h).wait_send()

            @pl.when(z < chain - 1)
            def _():
                copy_z(h).wait_send()

        return 0

    lax.fori_loop(0, groups, finish, 0)


def per_device(tokens, w_query, w_key, w_value, w_out):
    n_seq = lax.axis_size("seq")
    rows, width = tokens.shape
    heads = w_query.shape[1] // KEY_DIM
    groups = heads // PAIR
    chunk = min(256, rows)
    cols = w_out.shape[1] // lax.axis_size("head")
    vm = pltpu.VMEM
    slot = (heads, ROWS, VALUE_DIM)
    dma = pltpu.SemaphoreType.DMA
    return pl.pallas_call(
        functools.partial(kernel, n_seq, chunk),
        out_shape=jax.ShapeDtypeStruct((rows, cols), BF16),
        in_specs=[pl.BlockSpec(memory_space=pl.ANY)] * 5,
        out_specs=pl.BlockSpec(memory_space=pltpu.VMEM),
        scratch_shapes=[
            vm((rows, width), BF16),
            vm((width, 256), BF16),
            vm(w_value.shape, BF16),
            vm((w_out.shape[0], cols), BF16),
            vm((heads, rows, VALUE_DIM), BF16),
            vm((rows, 128), BF16),
            vm((128, rows), F32),
            vm((128, rows), F32),
            vm((heads, rows // chunk, ROWS, 2 * VALUE_DIM), F32),
            vm((heads, rows, 2 * VALUE_DIM), F32),
            vm((heads, rows, ROWS), BF16),
            vm((rows, w_out.shape[0]), BF16),
            vm(slot, F32), vm(slot, F32), vm(slot, F32),
            vm(slot, BF16), vm(slot, BF16), vm(slot, BF16), vm(slot, BF16), vm(slot, BF16), vm(slot, BF16),
            vm((rows, cols), F32),
            dma((3,)), dma((LOADS,)), dma((groups,)),
            dma((heads,)), dma((heads,)), dma((heads,)), dma((heads,)), dma((heads,)), dma((heads,)),
            dma((groups,)), dma((groups,)),
        ],
        compiler_params=pltpu.CompilerParams(
            collective_id=0, has_side_effects=True, vmem_limit_bytes=50 * 1024 * 1024
        ),
    )(tokens, w_query, w_key, w_value, w_out)


def solution(mesh):
    in_specs = (P("seq", None), P(None, "head"), P(None, "head"), P(None, "head"), P())
    return jax.shard_map(
        per_device, mesh=mesh, in_specs=in_specs, out_specs=P("seq", "head"), check_vma=False
    )
```
